256 devices in a mesh: expert: 8 (over x, core), shard: 32 (over z, y).
Axes of the slice: x: 4, y: 4, z: 8, core: 2. Of those that a mesh axis runs over, the one named last changes fastest.
Arguments:
- master_gate: float32 [128, 2048, 768], P('expert', 'shard'), may hold values from -0.125 to 0.125
- master_up: float32 [128, 2048, 768], P('expert', 'shard'), may hold values from -0.125 to 0.125
- router_weight: float32 [2048, 128], P('shard', 'expert'), may hold values from -0.125 to 0.125
- router_gain: float32 [2048], P('shard'), may hold values from 0.25 to 1.75
Outputs:
- final_gate: bfloat16 [128, 768, 2048], P('expert', 'shard')
- final_up: bfloat16 [128, 768, 2048], P('expert', 'shard')
- serve_router: bfloat16 [2048, 128], replicated
The draws below stay inside these ranges and needn't reach their ends.
All inputs are finite; a program needn't handle non-finite values.
Results may differ from the reference program's by a relative error of at most 0.001.
Values may be sent and summed in bfloat16 or wider, within the bound.
No kernel may reach another device: no remote copies, remote signals or barrier semaphores. Data moves between devices by JAX's collectives and lax.ppermute only.
A program may use at most 64 MiB of HBM per device.

```python
import jax
import jax.numpy as jnp

EXPERTS = 128
D_MODEL = 2048
D_EXPERT = 768


def shard_levels(key, extent, shards, least, largest):
    gain, own = 1.0, jax.random.fold_in(key, 6)
    for axis_at, shards_of in shards:
        heights = jnp.exp(jax.random.uniform(jax.random.fold_in(own, axis_at), (shards_of,), jnp.float32, least / len(shards), largest / len(shards)))
        gain = gain * jnp.repeat(heights, extent[axis_at] // shards_of).reshape([-1 if axis == axis_at else 1 for axis in range(len(extent))])
    return gain


def centred(key, extent, width, most, split=(), dtype=jnp.bfloat16):
    array = width * jax.random.normal(key, extent, jnp.float32)
    if split:
        array = array * shard_levels(key, extent, split, -0.22, 0.18)
    return jnp.clip(array, -most, most).astype(dtype)


def setup_inputs(seed: int = 0) -> dict:
    key_list = jax.random.split(jax.random.key(seed), 5)
    master_gate = centred(key_list[0], (EXPERTS, D_MODEL, D_EXPERT), D_MODEL ** -0.5, 0.125, ((0, 8), (1, 32)), jnp.float32)
    master_up = centred(key_list[1], (EXPERTS, D_MODEL, D_EXPERT), D_MODEL ** -0.5, 0.125, ((0, 8), (1, 32)), jnp.float32)
    router_weight = centred(key_list[2], (D_MODEL, EXPERTS), D_MODEL ** -0.5, 0.125, ((0, 32), (1, 8)), jnp.float32)
    router_gain = jnp.clip(1.0 + 0.15 * jax.random.normal(key_list[3], (D_MODEL,), jnp.float32), 0.25, 1.75)
    return {"master_gate": master_gate, "master_up": master_up, "router_weight": router_weight, "router_gain": router_gain}


def reference(master_gate, master_up, router_weight, router_gain):
    final_gate = master_gate.astype(jnp.bfloat16)
    final_gate = jnp.transpose(final_gate, (0, 2, 1))
    final_up = master_up.astype(jnp.bfloat16)
    final_up = jnp.transpose(final_up, (0, 2, 1))
    serve_router = (router_weight * router_gain[:, None]).astype(jnp.bfloat16)
    return final_gate, final_up, serve_router
```

```python
import functools

import jax
import jax.numpy as jnp
from jax import lax
from jax.experimental import pallas as pl
from jax.experimental.pallas import tpu as pltpu
from jax.sharding import Mesh
from jax.sharding import PartitionSpec as P

EXPERT = ("x", "core")
SHARD = ("z", "y")
RINGED = 6
LANES = 128
TILE = 8

VMEM = pl.BlockSpec(memory_space=pltpu.VMEM)
GRANT = pltpu.CompilerParams(vmem_limit_bytes=16 * 2**20)
RING_ORDER = (3, 5, 4, 2, 6, 1, 7)
SIDE_ORDER = (1, 3, 2)


def two_experts(master_ref):
    swap = lax.axis_index("y") % 2
    stacked = jnp.concatenate([master_ref[swap, 0], master_ref[1 - swap, 0]], axis=0)
    return stacked.astype(jnp.bfloat16).T


def merged_pairs(first, second):
    low = lax.broadcasted_iota(jnp.int32, first.shape, first.ndim - 1) < LANES // 2
    here = jnp.where(low, first, second)
    there = jnp.where(low, second, first)
    return here, jnp.concatenate([there[..., LANES // 2 :], there[..., : LANES // 2]], axis=-1)


def pack_ringed_kernel(zs, ys, own, master_ref, weight_ref, gain_ref, *refs):
    outs, rows_ref = refs[:zs], refs[zs]
    step = pl.program_id(0)
    z = lax.axis_index("z")
    rows_ref[...] = two_experts(master_ref)
    for dz in range(zs):
        start = lax.rem(z + dz, zs) * (ys * own)
        moved = rows_ref[pl.ds(pl.multiple_of(start, TILE), ys * own), :]
        for y in range(ys):
            row = pl.multiple_of((y * RINGED + step) * own, TILE)
            outs[dz][pl.ds(row, own), :] = moved[y * own : (y + 1) * own]

    @pl.when(step == 0)
    def _():
        part = (weight_ref[...] * gain_ref[...]).astype(jnp.bfloat16)
        tile = jnp.concatenate([part[:TILE], part[TILE:]], axis=1)
        for out in outs:
            out[-TILE:, :] = tile


def pack_ringed(master, weight, gain, zs, ys):
    _, _, depth, wide = master.shape
    own = wide // (zs * ys)
    return pl.pallas_call(
        functools.partial(pack_ringed_kernel, zs, ys, own),
        grid=(RINGED,),
        in_specs=[
            pl.BlockSpec((2, 1, depth, wide), lambda e: (0, e, 0, 0)),
            pl.BlockSpec(weight.shape, lambda e: (0, 0)),
            pl.BlockSpec(gain.shape, lambda e: (0, 0)),
        ],
        out_specs=[VMEM] * zs,
        out_shape=[jax.ShapeDtypeStruct((ys * RINGED * own + TILE, LANES), jnp.bfloat16)] * zs,
        scratch_shapes=[pltpu.VMEM((wide, LANES), jnp.bfloat16)],
        compiler_params=GRANT,
        cost_estimate=pl.CostEstimate(flops=10**8, bytes_accessed=10**7, transcendentals=0),
        name="pack_ringed",
    )(master, weight, gain)


def router_tiles_kernel(*refs):
    zs = len(refs) - 1
    z = lax.axis_index("z")
    for j in range(zs):
        refs[zs][lax.rem(z + zs - j, zs)] = refs[j][-TILE:, :]


def router_tiles(near):
    return pl.pallas_call(
        router_tiles_kernel,
        in_specs=[VMEM] * len(near),
        out_specs=VMEM,
        out_shape=jax.ShapeDtypeStruct((len(near), TILE, LANES), jnp.bfloat16),
        compiler_params=GRANT,
        name="router_tiles",
    )(*near)


def regroup_kernel(ys, *refs):
    zs = len(refs) - ys
    z, y = lax.axis_index("z"), lax.axis_index("y")
    rows = (refs[0].shape[0] - TILE) // ys
    for k in range(ys):
        start = pl.multiple_of(lax.rem(y + k, ys) * rows, TILE)
        for j in range(zs):
            refs[zs + k][lax.rem(z + zs - j, zs)] = refs[j][pl.ds(start, rows), :]


def regroup(near, ys):
    rows, lanes = near[0].shape
    shape = jax.ShapeDtypeStruct((len(near), (rows - TILE) // ys, lanes), jnp.bfloat16)
    return pl.pallas_call(
        functools.partial(regroup_kernel, ys),
        in_specs=[VMEM] * len(near),
        out_specs=[VMEM] * ys,
        out_shape=[shape] * ys,
        compiler_params=GRANT,
        name="regroup",
    )(*near)


def for_each_y(ys, write):
    y = lax.axis_index("y")
    for me in range(ys):

        @pl.when(y == me)
        def _():
            for even in range(0, ys, 2):
                write(even, (me - even) % ys, (me - even - 1) % ys)


def router_rows_kernel(*refs):
    out_ref = refs[-1]
    ys = len(refs) - 1

    def write(even, a, b):
        for z in range(refs[0].shape[0]):
            first, second = refs[a][z], refs[b][z]
            column = (z * ys + even) * (LANES // 2)
            out_ref[:TILE, column : column + LANES] = jnp.concatenate(
                [first[:, : LANES // 2], second[:, : LANES // 2]], axis=1
            )
            out_ref[TILE:, column : column + LANES] = jnp.concatenate(
                [first[:, LANES // 2 :], second[:, LANES // 2 :]], axis=1
            )

    for_each_y(ys, write)


def router_rows(tiles):
    zs, ys = tiles[0].shape[0], len(tiles)
    return pl.pallas_call(
        router_rows_kernel,
        in_specs=[VMEM] * ys,
        out_specs=VMEM,
        out_shape=jax.ShapeDtypeStruct((2 * TILE, zs * ys * LANES // 2), jnp.bfloat16),
        compiler_params=GRANT,
        name="router_rows",
    )(*tiles)


def unpack_ringed_kernel(own, *refs):
    out_ref = refs[-1]
    ys = len(refs) - 1
    rows = pl.ds(pl.multiple_of(pl.program_id(0) * own, TILE), own)

    def write(even, a, b):
        for z in range(refs[0].shape[0]):
            column = (z * ys + even) * (LANES // 2)
            here, there = merged_pairs(refs[a][z, rows, :], refs[b][z, rows, :])
            out_ref[0, 0, :, column : column + LANES] = here
            out_ref[1, 0, :, column : column + LANES] = there

    for_each_y(ys, write)


def unpack_ringed(groups, half, own):
    zs, ys = groups[0].shape[0], len(groups)
    depth = zs * ys * LANES // 2
    return pl.pallas_call(
        functools.partial(unpack_ringed_kernel, own),
        grid=(RINGED,),
        in_specs=[VMEM] * ys,
        out_specs=pl.BlockSpec((2, 1, own, depth), lambda e: (0, e, 0, 0)),
        out_shape=jax.ShapeDtypeStruct((2, half, own, depth), jnp.bfloat16),
        compiler_params=GRANT,
        cost_estimate=pl.CostEstimate(flops=10**8, bytes_accessed=10**7, transcendentals=0),
        name="unpack_ringed",
    )(*groups)


def pack_rest_kernel(left, shards, own, gate_ref, up_ref, out_ref):
    step = pl.program_id(0)
    rows = pl.ds(pl.multiple_of(step * own, TILE), own)

    @pl.when(step < left)
    def _():
        out_ref[:, rows, :] = two_experts(gate_ref).reshape(shards, own, LANES)

    @pl.when(step >= left)
    def _():
        out_ref[:, rows, :] = two_experts(up_ref).reshape(shards, own, LANES)


def pack_rest(gate, up, shards):
    _, half, depth, wide = gate.shape
    own, left = wide // shards, half - RINGED
    return pl.pallas_call(
        functools.partial(pack_rest_kernel, left, shards, own),
        grid=(left + half,),
        in_specs=[
            pl.BlockSpec((2, 1, depth, wide), lambda e: (0, jnp.minimum(RINGED + e, half - 1), 0, 0)),
            pl.BlockSpec((2, 1, depth, wide), lambda e: (0, jnp.maximum(e - left, 0), 0, 0)),
        ],
        out_specs=VMEM,
        out_shape=pltpu.HBM((shards, (left + half) * own, LANES), jnp.bfloat16),
        compiler_params=GRANT,
        cost_estimate=pl.CostEstimate(flops=10**8, bytes_accessed=10**7, transcendentals=0),
        name="pack_rest",
    )(gate, up)


def unpack_rest_kernel(left, own, in_ref, _, gate_ref, up_ref):
    step = pl.program_id(0)
    rows = pl.ds(pl.multiple_of(step * own, TILE), own)

    def write(out_ref):
        for k in range(in_ref.shape[0] // 2):
            here, there = merged_pairs(in_ref[2 * k, rows, :], in_ref[2 * k + 1, rows, :])
            out_ref[0, 0, :, k * LANES : (k + 1) * LANES] = here
            out_ref[1, 0, :, k * LANES : (k + 1) * LANES] = there

    @pl.when(step < left)
    def _():
        write(gate_ref)

    @pl.when(step >= left)
    def _():
        write(up_ref)


def unpack_rest(received, gate):
    _, half, own, depth = gate.shape
    left = half - RINGED
    return pl.pallas_call(
        functools.partial(unpack_rest_kernel, left, own),
        grid=(left + half,),
        in_specs=[VMEM, pl.BlockSpec(memory_space=pl.ANY)],
        out_specs=[
            pl.BlockSpec((2, 1, own, depth), lambda e: (0, jnp.minimum(RINGED + e, half - 1), 0, 0)),
            pl.BlockSpec((2, 1, own, depth), lambda e: (0, jnp.maximum(e - left, 0), 0, 0)),
        ],
        out_shape=[jax.ShapeDtypeStruct(gate.shape, jnp.bfloat16)] * 2,
        input_output_aliases={1: 0},
        compiler_params=GRANT,
        cost_estimate=pl.CostEstimate(flops=10**8, bytes_accessed=10**7, transcendentals=0),
        name="unpack_rest",
    )(received, gate)


def in_hbm(array):
    return pltpu.with_memory_space_constraint(array, pltpu.HBM)


def shifted(block, axis, by):
    size = lax.axis_size(axis)
    return lax.ppermute(block, axis, [(k, (k + by) % size) for k in range(size)])


def per_device(master_gate, master_up, router_weight, router_gain):
    zs, ys = lax.axis_size("z"), lax.axis_size("y")
    experts, depth, wide = master_gate.shape
    half, own = experts // 2, wide // (zs * ys)
    gate, up = (m.reshape(2, half, depth, wide) for m in (master_gate, master_up))
    gate = in_hbm(gate)
    weight, gain = in_hbm(router_weight.T), in_hbm(router_gain[None])
    near = list(pack_ringed(gate, weight, gain, zs, ys))
    for dz in RING_ORDER:
        near[dz] = shifted(near[dz], "z", dz)
    rest = pack_rest(gate, up, zs * ys)
    got_rest = lax.all_to_all(rest, SHARD, 0, 0, tiled=True)
    tiles = [router_tiles(near)] * ys
    for dy in SIDE_ORDER:
        tiles[dy] = shifted(tiles[dy], "y", dy)
    groups = list(regroup(near, ys))
    for dy in SIDE_ORDER:
        groups[dy] = shifted(groups[dy], "y", dy)
    everyone = lax.all_gather(router_rows(tiles), EXPERT, axis=0, tiled=True)
    serve_router = everyone.T
    final_gate = unpack_ringed(groups, half, own)
    final_gate, final_up = unpack_rest(got_rest, final_gate)
    whole = (experts, own, zs * ys * depth)
    return final_gate.reshape(whole), final_up.reshape(whole), serve_router


def solution(mesh):
    torus = Mesh(mesh.devices.reshape(4, 2, 8, 4), ("x", "core", "z", "y"))
    return jax.shard_map(
        per_device,
        mesh=torus,
        in_specs=(P(EXPERT, SHARD, None), P(EXPERT, SHARD, None), P(SHARD, EXPERT), P(SHARD)),
        out_specs=(P(EXPERT, SHARD, None), P(EXPERT, SHARD, None), P()),
        check_vma=False,
    )
```

```python
import functools

import jax
import jax.numpy as jnp
from jax import lax
from jax.experimental import pallas as pl
from jax.experimental.pallas import tpu as pltpu
from jax.sharding import Mesh
from jax.sharding import PartitionSpec as P

EXPERT = ("x", "core")
SHARD = ("z", "y")
RINGED = 7
LANES = 128
TILE = 8

VMEM = pl.BlockSpec(memory_space=pltpu.VMEM)
HBM = pl.BlockSpec(memory_space=pl.ANY)
GRANT = pltpu.CompilerParams(vmem_limit_bytes=16 * 2**20)
RING = (4, 3, 5, 2, 6, 1, 7)
LATER = (0,) + RING[1:]
SIDES = (1, 3, 2)


def cost(size):
    return pl.CostEstimate(flops=10**8, bytes_accessed=size, transcendentals=0)


def packed(rows):
    return jax.ShapeDtypeStruct(rows, jnp.bfloat16)


def two_experts(unit_ref):
    swap = lax.axis_index("y") % 2
    stacked = jnp.concatenate([unit_ref[swap], unit_ref[1 - swap]], axis=0)
    return stacked.astype(jnp.bfloat16).T


def merged_pairs(first, second):
    low = lax.broadcasted_iota(jnp.int32, first.shape, first.ndim - 1) < LANES // 2
    here = jnp.where(low, first, second)
    there = jnp.where(low, second, first)
    return here, jnp.concatenate([there[..., LANES // 2 :], there[..., : LANES // 2]], axis=-1)


def fetched(sources, units_ref, sems):
    copies = [pltpu.make_async_copy(source, units_ref.at[n], sems.at[n]) for n, source in enumerate(sources)]
    for copy in copies:
        copy.start()
    for n, copy in enumerate(copies):
        copy.wait()
        yield n, two_experts(units_ref.at[n])


def router_tile(weight_ref, gain_ref):
    part = (weight_ref[...] * gain_ref[...]).astype(jnp.bfloat16)
    return jnp.concatenate([part[:TILE], part[TILE:]], axis=1)


def pack_first_kernel(zs, ys, own, master_ref, weight_ref, gain_ref, out_ref, units_ref, rows_ref, sems):
    out_ref[-TILE:, :] = router_tile(weight_ref, gain_ref)
    width = units_ref.shape[-1]
    first = lax.rem(lax.axis_index("z") + RING[0], zs) * (ys * own)
    base = jnp.minimum(first // LANES * LANES, zs * ys * own - width)
    columns = pl.ds(pl.multiple_of(base, LANES), width)
    for e, rows in fetched([master_ref.at[:, e, :, columns] for e in range(RINGED)], units_ref, sems):
        rows_ref[e % 2] = rows
        moved = rows_ref[e % 2, pl.ds(pl.multiple_of(first - base, TILE), ys * own), :]
        for y in range(ys):
            row = (y * RINGED + e) * own
            out_ref[row : row + own, :] = moved[y * own : (y + 1) * own]


def pack_ringed_kernel(zs, ys, own, master_ref, weight_ref, gain_ref, *refs):
    outs, (units_ref, rows_ref, sems) = refs[:-3], refs[-3:]
    z = lax.axis_index("z")
    tile = router_tile(weight_ref, gain_ref)
    for out in outs:
        out[-TILE:, :] = tile
    for e, rows in fetched([master_ref.at[:, e] for e in range(RINGED)], units_ref, sems):
        rows_ref[e % 2] = rows
        for dz, out in zip(LATER, outs):
            start = lax.rem(z + dz, zs) * (ys * own)
            moved = rows_ref[e % 2, pl.ds(pl.multiple_of(start, TILE), ys * own), :]
            for y in range(ys):
                row = (y * RINGED + e) * own
                out[row : row + own, :] = moved[y * own : (y + 1) * own]


def pack_for(kernel, outs, width, master, weight, gain, zs, ys):
    _, _, depth, wide = master.shape
    own = wide // (zs * ys)
    return pl.pallas_call(
        functools.partial(kernel, zs, ys, own),
        in_specs=[HBM, VMEM, VMEM],
        out_specs=[VMEM] * outs,
        out_shape=[packed((ys * RINGED * own + TILE, LANES))] * outs,
        scratch_shapes=[
            pltpu.VMEM((RINGED, 2, depth, width), jnp.float32),
            pltpu.VMEM((2, width, LANES), jnp.bfloat16),
            pltpu.SemaphoreType.DMA((RINGED,)),
        ],
        compiler_params=GRANT,
        cost_estimate=cost(4 * master.size),
    )(master, weight, gain)


def pack_ring(master, weight, gain, zs, ys):
    wide = master.shape[-1]
    width = -(-(wide // zs + LANES - TILE) // LANES) * LANES
    (first,) = pack_for(pack_first_kernel, 1, width, master, weight, gain, zs, ys)
    later = pack_for(pack_ringed_kernel, len(LATER), wide, master, weight, gain, zs, ys)
    near = dict(zip(LATER, later))
    near[RING[0]] = first
    return [near[dz] for dz in range(zs)]


def router_tiles_kernel(*refs):
    zs = len(refs) - 1
    z = lax.axis_index("z")
    for j in range(zs):
        refs[zs][lax.rem(z + zs - j, zs)] = refs[j][-TILE:, :]


def router_tiles(near):
    return pl.pallas_call(
        router_tiles_kernel,
        in_specs=[pl.BlockSpec((TILE, LANES), lambda e: (near[0].shape[0] // TILE - 1, 0))] * len(near),
        out_specs=VMEM,
        out_shape=packed((len(near), TILE, LANES)),
        grid=(1,),
        compiler_params=GRANT,
        name="router_tiles",
    )(*near)


def regroup_kernel(ys, *refs):
    zs = len(refs) - ys
    z, y = lax.axis_index("z"), lax.axis_index("y")
    rows = (refs[0].shape[0] - TILE) // ys
    for k in range(ys):
        start = pl.multiple_of(lax.rem(y + k, ys) * rows, TILE)
        for j in range(zs):
            refs[zs + k][lax.rem(z + zs - j, zs)] = refs[j][pl.ds(start, rows), :]


def regroup(near, ys):
    rows, lanes = near[0].shape
    shape = jax.ShapeDtypeStruct((len(near), (rows - TILE) // ys, lanes), jnp.bfloat16)
    return pl.pallas_call(
        functools.partial(regroup_kernel, ys),
        in_specs=[VMEM] * len(near),
        out_specs=[VMEM] * ys,
        out_shape=[shape] * ys,
        compiler_params=GRANT,
        name="regroup",
    )(*near)


def router_rows_kernel(*refs):
    out_ref = refs[-1]
    ys = len(refs) - 1
    y = lax.axis_index("y")

    def write(me):
        for even in range(0, ys, 2):
            a, b = (me - even) % ys, (me - even - 1) % ys
            for z in range(refs[0].shape[0]):
                first, second = refs[a][z], refs[b][z]
                column = (z * ys + even) * (LANES // 2)
                out_ref[:TILE, column : column + LANES] = jnp.concatenate(
                    [first[:, : LANES // 2], second[:, : LANES // 2]], axis=1
                )
                out_ref[TILE:, column : column + LANES] = jnp.concatenate(
                    [first[:, LANES // 2 :], second[:, LANES // 2 :]], axis=1
                )

    for me in range(ys):
        pl.when(y == me)(functools.partial(write, me))


def router_rows(tiles):
    zs, ys = tiles[0].shape[0], len(tiles)
    return pl.pallas_call(
        router_rows_kernel,
        in_specs=[VMEM] * ys,
        out_specs=VMEM,
        out_shape=packed((2 * TILE, zs * ys * LANES // 2)),
        compiler_params=GRANT,
        name="router_rows",
    )(*tiles)


def sent(targets, units_ref, sems, own, write):
    copies = []
    for n, target in enumerate(targets):
        write(units_ref.at[n], slice(n * own, (n + 1) * own))
        copies.append(pltpu.make_async_copy(units_ref.at[n], target, sems.at[n]))
        copies[-1].start()
    for copy in copies:
        copy.wait()


def unpack_ringed_kernel(own, *refs):
    groups, (out_ref, ordered_ref, units_ref, sems) = refs[:-4], refs[-4:]
    ys, zs = ordered_ref.shape[:2]
    y = lax.axis_index("y")
    for k, group in enumerate(groups):
        ordered_ref[lax.rem(y + ys - k, ys)] = group[...]

    def write(unit_ref, rows):
        for z in range(zs):
            for even in range(0, ys, 2):
                column = (z * ys + even) * (LANES // 2)
                here, there = merged_pairs(ordered_ref[even, z, rows, :], ordered_ref[even + 1, z, rows, :])
                unit_ref[0, :, column : column + LANES] = here
                unit_ref[1, :, column : column + LANES] = there

    sent([out_ref.at[:, e] for e in range(RINGED)], units_ref, sems, own, write)


def unpack_ringed(groups, half, own):
    zs, ys = groups[0].shape[0], len(groups)
    depth = zs * ys * LANES // 2
    return pl.pallas_call(
        functools.partial(unpack_ringed_kernel, own),
        in_specs=[VMEM] * ys,
        out_specs=HBM,
        out_shape=pltpu.HBM((2, half, own, depth), jnp.bfloat16),
        scratch_shapes=[
            pltpu.VMEM((ys, *groups[0].shape), jnp.bfloat16),
            pltpu.VMEM((RINGED, 2, own, depth), jnp.bfloat16),
            pltpu.SemaphoreType.DMA((RINGED,)),
        ],
        compiler_params=GRANT,
        cost_estimate=cost(8 * half * own * depth),
        name="unpack_ringed",
    )(*groups)


def rest_of(gate_ref, up_ref, half):
    return [gate_ref.at[:, e] for e in range(RINGED, half)] + [up_ref.at[:, e] for e in range(half)]


def pack_rest_kernel(shards, own, gate_ref, up_ref, out_ref, units_ref, rows_ref, sems, out_sems):
    copies = []
    for n, moved in fetched(rest_of(gate_ref, up_ref, gate_ref.shape[1]), units_ref, sems):
        rows = slice(n * own, (n + 1) * own)
        rows_ref[:, rows, :] = moved.reshape(shards, own, LANES)
        copies.append(pltpu.make_async_copy(rows_ref.at[:, rows], out_ref.at[:, rows], out_sems.at[n]))
        copies[-1].start()
    for copy in copies:
        copy.wait()


def pack_rest(gate, up, shards):
    _, half, depth, wide = gate.shape
    own, count = wide // shards, 2 * half - RINGED
    shape = (shards, count * own, LANES)
    return pl.pallas_call(
        functools.partial(pack_rest_kernel, shards, own),
        in_specs=[HBM] * 2,
        out_specs=HBM,
        out_shape=pltpu.HBM(shape, jnp.bfloat16),
        scratch_shapes=[
            pltpu.VMEM((count, 2, depth, wide), jnp.float32),
            pltpu.VMEM(shape, jnp.bfloat16),
            pltpu.SemaphoreType.DMA((count,)),
            pltpu.SemaphoreType.DMA((count,)),
        ],
        compiler_params=GRANT,
        cost_estimate=cost(8 * gate.size),
        name="pack_rest",
    )(gate, up)


def unpack_rest_kernel(own, in_ref, _, gate_ref, up_ref, units_ref, sems):
    def write(unit_ref, rows):
        for k in range(in_ref.shape[0] // 2):
            here, there = merged_pairs(in_ref[2 * k, rows, :], in_ref[2 * k + 1, rows, :])
            unit_ref[0, :, k * LANES : (k + 1) * LANES] = here
            unit_ref[1, :, k * LANES : (k + 1) * LANES] = there

    sent(rest_of(gate_ref, up_ref, gate_ref.shape[1]), units_ref, sems, own, write)


def unpack_rest(received, gate):
    _, half, own, depth = gate.shape
    count = 2 * half - RINGED
    return pl.pallas_call(
        functools.partial(unpack_rest_kernel, own),
        in_specs=[VMEM, HBM],
        out_specs=[HBM] * 2,
        out_shape=[pltpu.HBM(gate.shape, jnp.bfloat16)] * 2,
        scratch_shapes=[
            pltpu.VMEM((count, 2, own, depth), jnp.bfloat16),
            pltpu.SemaphoreType.DMA((count,)),
        ],
        input_output_aliases={1: 0},
        compiler_params=GRANT,
        cost_estimate=cost(8 * gate.size),
        name="unpack_rest",
    )(received, gate)


def in_hbm(array):
    return pltpu.with_memory_space_constraint(array, pltpu.HBM)


def shifted(block, axis, by):
    size = lax.axis_size(axis)
    return lax.ppermute(block, axis, [(k, (k + by) % size) for k in range(size)])


def per_device(master_gate, master_up, router_weight, router_gain):
    zs, ys = lax.axis_size("z"), lax.axis_size("y")
    experts, depth, wide = master_gate.shape
    half, own = experts // 2, wide // (zs * ys)
    gate, up = (m.reshape(2, half, depth, wide) for m in (master_gate, master_up))
    gate, up = in_hbm(gate), in_hbm(up)
    weight, gain = in_hbm(router_weight.T), in_hbm(router_gain[None])
    near = pack_ring(gate, weight, gain, zs, ys)
    for dz in RING:
        near[dz] = shifted(near[dz], "z", dz)
    rest = pack_rest(gate, up, zs * ys)
    got_rest = lax.all_to_all(rest, SHARD, 0, 0, tiled=True)
    tiles = [router_tiles(near)] * ys
    for dy in SIDES:
        tiles[dy] = shifted(tiles[dy], "y", dy)
    groups = list(regroup(near, ys))
    for dy in SIDES:
        groups[dy] = shifted(groups[dy], "y", dy)
    everyone = lax.all_gather(router_rows(tiles), EXPERT, axis=0, tiled=True)
    serve_router = everyone.T
    final_gate = unpack_ringed(groups, half, own)
    final_gate, final_up = unpack_rest(got_rest, final_gate)
    whole = (experts, own, zs * ys * depth)
    return final_gate.reshape(whole), final_up.reshape(whole), serve_router


def solution(mesh):
    torus = Mesh(mesh.devices.reshape(4, 2, 8, 4), ("x", "core", "z", "y"))
    return jax.shard_map(
        per_device,
        mesh=torus,
        in_specs=(P(EXPERT, SHARD, None), P(EXPERT, SHARD, None), P(SHARD, EXPERT), P(SHARD)),
        out_specs=(P(EXPERT, SHARD, None), P(EXPERT, SHARD, None), P()),
        check_vma=False,
    )
```

```python
import functools

import jax
import jax.numpy as jnp
from jax import lax
from jax.experimental import pallas as pl
from jax.experimental.pallas import tpu as pltpu
from jax.sharding import Mesh
from jax.sharding import PartitionSpec as P

EXPERT = ("x", "core")
SHARD = ("z", "y")
LANES = 128
TILE = 8
CHUNK = 48

VMEM = pl.BlockSpec(memory_space=pltpu.VMEM)
HBM = pl.BlockSpec(memory_space=pl.ANY)
GRANT = pltpu.CompilerParams(vmem_limit_bytes=16 * 2**20)
RING = (4, 1, 7, 3, 5, 2, 6)
BATCHES = ((0, 4, 1, 7), (3, 5, 2, 6))
LATER = (0,) + RING[1:]
SIDES = (1, 3, 2)


def cost(size):
    return pl.CostEstimate(flops=10**8, bytes_accessed=size, transcendentals=0)


def packed(rows):
    return jax.ShapeDtypeStruct(rows, jnp.bfloat16)


def two_experts(unit_ref):
    swap = lax.axis_index("y") % 2
    stacked = jnp.concatenate([unit_ref[swap], unit_ref[1 - swap]], axis=0)
    return stacked.astype(jnp.bfloat16).T


def merged_pairs(first, second):
    low = lax.broadcasted_iota(jnp.int32, first.shape, first.ndim - 1) < LANES // 2
    here = jnp.where(low, first, second)
    there = jnp.where(low, second, first)
    return here, jnp.concatenate([there[..., LANES // 2 :], there[..., : LANES // 2]], axis=-1)


def fetched(sources, units_ref, sems, beside=None):
    copies = [pltpu.make_async_copy(source, units_ref.at[n], sems.at[n]) for n, source in enumerate(sources)]
    for copy in copies:
        copy.start()
    if beside is not None:
        next(beside)
    for n, copy in enumerate(copies):
        copy.wait()
        yield n, two_experts(units_ref.at[n])


def router_tile(router_refs, held_refs, sems):
    copies = [pltpu.make_async_copy(a, b, sems.at[n]) for n, (a, b) in enumerate(zip(router_refs, held_refs))]
    for copy in copies:
        copy.start()
    yield
    for copy in copies:
        copy.wait()
    part = (held_refs[0][...] * held_refs[1][...]).astype(jnp.bfloat16)
    yield jnp.concatenate([part[:TILE], part[TILE:]], axis=1)


def pack_first_kernel(zs, ys, own, master_ref, *refs):
    (out_ref,), (units_ref, rows_ref, sems, *held, held_sems) = refs[2:3], refs[3:]
    width = units_ref.shape[-1]
    first = lax.rem(lax.axis_index("z") + RING[0], zs) * (ys * own)
    base = jnp.minimum(first // LANES * LANES, zs * ys * own - width)
    columns = pl.ds(pl.multiple_of(base, LANES), width)
    sources = [master_ref.at[:, e, :, columns] for e in range(units_ref.shape[0])]
    tile = router_tile(refs[:2], held, held_sems)
    for e, rows in fetched(sources, units_ref, sems, tile):
        rows_ref[e % 2] = rows
        moved = rows_ref[e % 2, pl.ds(pl.multiple_of(first - base, TILE), ys * own), :]
        for y in range(ys):
            row = (y * units_ref.shape[0] + e) * own
            out_ref[row : row + own, :] = moved[y * own : (y + 1) * own]
    out_ref[-TILE:, :] = next(tile)


def pack_ringed_kernel(zs, ys, own, master_ref, *refs):
    outs, (units_ref, rows_ref, sems, *held, held_sems) = refs[2 : 2 + len(LATER)], refs[2 + len(LATER) :]
    z = lax.axis_index("z")
    tile = router_tile(refs[:2], held, held_sems)
    for e, rows in fetched([master_ref.at[:, e] for e in range(units_ref.shape[0])], units_ref, sems, tile):
        rows_ref[e % 2] = rows
        for dz, out in zip(LATER, outs):
            start = lax.rem(z + dz, zs) * (ys * own)
            moved = rows_ref[e % 2, pl.ds(pl.multiple_of(start, TILE), ys * own), :]
            for y in range(ys):
                row = (y * units_ref.shape[0] + e) * own
                out[row : row + own, :] = moved[y * own : (y + 1) * own]
    tile = next(tile)
    for out in outs:
        out[-TILE:, :] = tile


def pack_for(kernel, outs, width, master, weight, gain, zs, ys):
    _, half, depth, wide = master.shape
    own = wide // (zs * ys)
    return pl.pallas_call(
        functools.partial(kernel, zs, ys, own),
        in_specs=[HBM] * 3,
        out_specs=[VMEM] * outs,
        out_shape=[packed((ys * half * own + TILE, LANES))] * outs,
        scratch_shapes=[
            pltpu.VMEM((half, 2, depth, width), jnp.float32),
            pltpu.VMEM((2, width, LANES), jnp.bfloat16),
            pltpu.SemaphoreType.DMA((half,)),
            pltpu.VMEM(weight.shape, jnp.float32),
            pltpu.VMEM(gain.shape, jnp.float32),
            pltpu.SemaphoreType.DMA((2,)),
        ],
        compiler_params=GRANT,
        cost_estimate=cost(4 * master.size),
    )(master, weight, gain)


def pack_ring(master, weight, gain, zs, ys):
    wide = master.shape[-1]
    width = -(-(wide // zs + LANES - TILE) // LANES) * LANES
    (first,) = pack_for(pack_first_kernel, 1, width, master, weight, gain, zs, ys)
    later = pack_for(pack_ringed_kernel, len(LATER), wide, master, weight, gain, zs, ys)
    near = dict(zip(LATER, later))
    near[RING[0]] = first
    return [near[dz] for dz in range(zs)]


def router_tiles_kernel(*refs):
    zs = len(refs) - 1
    z = lax.axis_index("z")
    for j in range(zs):
        refs[zs][lax.rem(z + zs - j, zs)] = refs[j][-TILE:, :]


def router_tiles(near):
    return pl.pallas_call(
        router_tiles_kernel,
        in_specs=[pl.BlockSpec((TILE, LANES), lambda e: (near[0].shape[0] // TILE - 1, 0))] * len(near),
        out_specs=VMEM,
        out_shape=packed((len(near), TILE, LANES)),
        grid=(1,),
        compiler_params=GRANT,
        name="router_tiles",
    )(*near)


def regroup_kernel(ys, *refs):
    count = len(refs) - ys
    y = lax.axis_index("y")
    rows = refs[count].shape[1]
    for k in range(ys):
        start = pl.multiple_of(lax.rem(y + k, ys) * rows, TILE)
        for n in range(count):
            refs[count + k][n] = refs[n][pl.ds(start, rows), :]


def regroup(near, ys):
    rows, lanes = near[0].shape
    shape = packed((len(near), (rows - TILE) // ys, lanes))
    return pl.pallas_call(
        functools.partial(regroup_kernel, ys),
        in_specs=[VMEM] * len(near),
        out_specs=[VMEM] * ys,
        out_shape=[shape] * ys,
        compiler_params=GRANT,
    )(*near)


def router_rows_kernel(*refs):
    out_ref = refs[-1]
    ys = len(refs) - 1
    y = lax.axis_index("y")

    def write(me):
        for even in range(0, ys, 2):
            a, b = (me - even) % ys, (me - even - 1) % ys
            for z in range(refs[0].shape[0]):
                first, second = refs[a][z], refs[b][z]
                column = (z * ys + even) * (LANES // 2)
                out_ref[:TILE, column : column + LANES] = jnp.concatenate(
                    [first[:, : LANES // 2], second[:, : LANES // 2]], axis=1
                )
                out_ref[TILE:, column : column + LANES] = jnp.concatenate(
                    [first[:, LANES // 2 :], second[:, LANES // 2 :]], axis=1
                )

    for me in range(ys):
        pl.when(y == me)(functools.partial(write, me))


def router_rows(tiles):
    zs, ys = tiles[0].shape[0], len(tiles)
    return pl.pallas_call(
        router_rows_kernel,
        in_specs=[VMEM] * ys,
        out_specs=VMEM,
        out_shape=packed((2 * TILE, zs * ys * LANES // 2)),
        compiler_params=GRANT,
        name="router_rows",
    )(*tiles)


def sent(out_ref, units_ref, sems, write):
    count, _, rows, _ = units_ref.shape
    copies = []
    for n in range(count):
        part = slice(n * rows, (n + 1) * rows)
        write(units_ref.at[n], part)
        copies.append(pltpu.make_async_copy(units_ref.at[n], out_ref.at[:, part], sems.at[n]))
        copies[-1].start()
    for copy in copies:
        copy.wait()


def unpack(kernel, operands, scratch, rows, depth):
    return pl.pallas_call(
        kernel,
        in_specs=[VMEM] * len(operands),
        out_specs=HBM,
        out_shape=pltpu.HBM((2, rows, depth), jnp.bfloat16),
        scratch_shapes=[
            *scratch,
            pltpu.VMEM((rows // CHUNK, 2, CHUNK, depth), jnp.bfloat16),
            pltpu.SemaphoreType.DMA((rows // CHUNK,)),
        ],
        compiler_params=GRANT,
        cost_estimate=cost(8 * rows * depth),
    )(*operands)


def unpack_ringed_kernel(*refs):
    groups, (out_ref, ordered_ref, units_ref, sems) = refs[:-4], refs[-4:]
    ys, zs = ordered_ref.shape[:2]
    z, y = lax.axis_index("z"), lax.axis_index("y")
    for n, group in enumerate(groups):
        for place, dz in enumerate(BATCHES[n // ys]):
            ordered_ref[lax.rem(y + ys - n % ys, ys), lax.rem(z + zs - dz, zs)] = group[place]

    def write(unit_ref, part):
        for z in range(zs):
            for even in range(0, ys, 2):
                column = (z * ys + even) * (LANES // 2)
                here, there = merged_pairs(ordered_ref[even, z, part, :], ordered_ref[even + 1, z, part, :])
                unit_ref[0, :, column : column + LANES] = here
                unit_ref[1, :, column : column + LANES] = there

    sent(out_ref, units_ref, sems, write)


def unpack_rest_kernel(in_ref, out_ref, units_ref, sems):
    def write(unit_ref, part):
        for k in range(in_ref.shape[0] // 2):
            here, there = merged_pairs(in_ref[2 * k, part, :], in_ref[2 * k + 1, part, :])
            unit_ref[0, :, k * LANES : (k + 1) * LANES] = here
            unit_ref[1, :, k * LANES : (k + 1) * LANES] = there

    sent(out_ref, units_ref, sems, write)


def pack_rest_kernel(shards, own, up_ref, out_ref, units_ref, rows_ref, sems, out_sems):
    copies = []
    half = up_ref.shape[1]
    for n, moved in fetched([up_ref.at[:, e] for e in range(half)], units_ref, sems):
        rows = slice(n * own, (n + 1) * own)
        rows_ref[:, rows, :] = moved.reshape(shards, own, LANES)
        copies.append(pltpu.make_async_copy(rows_ref.at[:, rows], out_ref.at[:, rows], out_sems.at[n]))
        copies[-1].start()
    for copy in copies:
        copy.wait()


def pack_rest(up, shards):
    _, half, depth, wide = up.shape
    own = wide // shards
    shape = (shards, half * own, LANES)
    return pl.pallas_call(
        functools.partial(pack_rest_kernel, shards, own),
        in_specs=[HBM],
        out_specs=HBM,
        out_shape=pltpu.HBM(shape, jnp.bfloat16),
        scratch_shapes=[
            pltpu.VMEM((half, 2, depth, wide), jnp.float32),
            pltpu.VMEM(shape, jnp.bfloat16),
            pltpu.SemaphoreType.DMA((half,)),
            pltpu.SemaphoreType.DMA((half,)),
        ],
        compiler_params=GRANT,
        cost_estimate=cost(6 * up.size),
        name="pack_rest",
    )(up)


def in_hbm(array):
    return pltpu.with_memory_space_constraint(array, pltpu.HBM)


def shifted(block, axis, by):
    size = lax.axis_size(axis)
    return lax.ppermute(block, axis, [(k, (k + by) % size) for k in range(size)])


def per_device(master_gate, master_up, router_weight, router_gain):
    zs, ys = lax.axis_size("z"), lax.axis_size("y")
    experts, depth, wide = master_gate.shape
    half, own = experts // 2, wide // (zs * ys)
    gate, up = (m.reshape(2, half, depth, wide) for m in (master_gate, master_up))
    gate, up = in_hbm(gate), in_hbm(up)
    weight, gain = in_hbm(router_weight.T), in_hbm(router_gain[None])
    near = pack_ring(gate, weight, gain, zs, ys)
    for dz in RING:
        near[dz] = shifted(near[dz], "z", dz)
    rest = pack_rest(up, zs * ys)
    got_rest = lax.all_to_all(rest, SHARD, 0, 0, tiled=True)
    tiles = [router_tiles(near)] * ys
    for dy in SIDES:
        tiles[dy] = shifted(tiles[dy], "y", dy)
    groups = []
    for batch in BATCHES:
        group = list(regroup([near[dz] for dz in batch], ys))
        for dy in SIDES:
            group[dy] = shifted(group[dy], "y", dy)
        groups += group
    everyone = lax.all_gather(router_rows(tiles), EXPERT, axis=0, tiled=True)
    serve_router = everyone.T
    rows, width = half * own, zs * ys * depth
    ordered = [pltpu.VMEM((ys, zs, rows, LANES), jnp.bfloat16)]
    final_gate = unpack(unpack_ringed_kernel, groups, ordered, rows, width)
    final_up = unpack(unpack_rest_kernel, [got_rest], [], rows, width)
    whole = (experts, own, zs * ys * depth)
    return final_gate.reshape(whole), final_up.reshape(whole), serve_router


def solution(mesh):
    torus = Mesh(mesh.devices.reshape(4, 2, 8, 4), ("x", "core", "z", "y"))
    return jax.shard_map(
        per_device,
        mesh=torus,
        in_specs=(P(EXPERT, SHARD, None), P(EXPERT, SHARD, None), P(SHARD, EXPERT), P(SHARD)),
        out_specs=(P(EXPERT, SHARD, None), P(EXPERT, SHARD, None), P()),
        check_vma=False,
    )
```

```python
import functools

import jax
import jax.numpy as jnp
from jax import lax
from jax.experimental import pallas as pl
from jax.experimental.pallas import tpu as pltpu
from jax.sharding import Mesh
from jax.sharding import PartitionSpec as P

EXPERT = ("x", "core")
SHARD = ("z", "y")
LANES = 128
TILE = 8
CHUNK = 48

VMEM = pl.BlockSpec(memory_space=pltpu.VMEM)
HBM = pl.BlockSpec(memory_space=pl.ANY)
GRANT = pltpu.CompilerParams(vmem_limit_bytes=16 * 2**20)
RING = (4, 1, 7, 3, 5, 2, 6)
BATCHES = ((0, 4, 1, 7), (3, 5, 2, 6))
LATER = (0,) + RING[1:]
SIDES = (2, 1, 3)


def cost(size):
    return pl.CostEstimate(flops=10**8, bytes_accessed=size, transcendentals=0)


def packed(rows):
    return jax.ShapeDtypeStruct(rows, jnp.bfloat16)


def two_experts(unit_ref):
    swap = lax.axis_index("y") % 2
    stacked = jnp.concatenate([unit_ref[swap], unit_ref[1 - swap]], axis=0)
    return stacked.astype(jnp.bfloat16).T


def merged_pairs(first, second):
    low = lax.broadcasted_iota(jnp.int32, first.shape, first.ndim - 1) < LANES // 2
    here = jnp.where(low, first, second)
    there = jnp.where(low, second, first)
    return here, jnp.concatenate([there[..., LANES // 2 :], there[..., : LANES // 2]], axis=-1)


def fetched(sources, units_ref, sems, beside=None):
    copies = [pltpu.make_async_copy(source, units_ref.at[n], sems.at[n]) for n, source in enumerate(sources)]
    for copy in copies:
        copy.start()
    if beside is not None:
        next(beside)
    for n, copy in enumerate(copies):
        copy.wait()
        yield n, two_experts(units_ref.at[n])


def router_tile(router_refs, held_refs, sems):
    copies = [pltpu.make_async_copy(a, b, sems.at[n]) for n, (a, b) in enumerate(zip(router_refs, held_refs))]
    for copy in copies:
        copy.start()
    yield
    for copy in copies:
        copy.wait()
    part = (held_refs[0][...] * held_refs[1][...]).astype(jnp.bfloat16)
    yield jnp.concatenate([part[:TILE], part[TILE:]], axis=1)


def pack_first_kernel(zs, ys, own, master_ref, *refs):
    (out_ref,), (units_ref, rows_ref, sems, *held, held_sems) = refs[2:3], refs[3:]
    width = units_ref.shape[-1]
    first = lax.rem(lax.axis_index("z") + RING[0], zs) * (ys * own)
    base = jnp.minimum(first // LANES * LANES, zs * ys * own - width)
    columns = pl.ds(pl.multiple_of(base, LANES), width)
    sources = [master_ref.at[:, e, :, columns] for e in range(units_ref.shape[0])]
    tile = router_tile(refs[:2], held, held_sems)
    for e, rows in fetched(sources, units_ref, sems, tile):
        rows_ref[e % 2] = rows
        moved = rows_ref[e % 2, pl.ds(pl.multiple_of(first - base, TILE), ys * own), :]
        for y in range(ys):
            row = (y * units_ref.shape[0] + e) * own
            out_ref[row : row + own, :] = moved[y * own : (y + 1) * own]
    out_ref[-TILE:, :] = next(tile)


def pack_ringed_kernel(zs, ys, own, master_ref, *refs):
    outs, (units_ref, rows_ref, sems, *held, held_sems) = refs[2 : 2 + len(LATER)], refs[2 + len(LATER) :]
    z = lax.axis_index("z")
    tile = router_tile(refs[:2], held, held_sems)
    for e, rows in fetched([master_ref.at[:, e] for e in range(units_ref.shape[0])], units_ref, sems, tile):
        rows_ref[e % 2] = rows
        for dz, out in zip(LATER, outs):
            start = lax.rem(z + dz, zs) * (ys * own)
            moved = rows_ref[e % 2, pl.ds(pl.multiple_of(start, TILE), ys * own), :]
            for y in range(ys):
                row = (y * units_ref.shape[0] + e) * own
                out[row : row + own, :] = moved[y * own : (y + 1) * own]
    tile = next(tile)
    for out in outs:
        out[-TILE:, :] = tile


def pack_for(kernel, outs, width, master, weight, gain, zs, ys):
    _, half, depth, wide = master.shape
    own = wide // (zs * ys)
    return pl.pallas_call(
        functools.partial(kernel, zs, ys, own),
        in_specs=[HBM] * 3,
        out_specs=[VMEM] * outs,
        out_shape=[packed((ys * half * own + TILE, LANES))] * outs,
        scratch_shapes=[
            pltpu.VMEM((half, 2, depth, width), jnp.float32),
            pltpu.VMEM((2, width, LANES), jnp.bfloat16),
            pltpu.SemaphoreType.DMA((half,)),
            pltpu.VMEM(weight.shape, jnp.float32),
            pltpu.VMEM(gain.shape, jnp.float32),
            pltpu.SemaphoreType.DMA((2,)),
        ],
        compiler_params=GRANT,
        cost_estimate=cost(4 * master.size),
    )(master, weight, gain)


def pack_ring(master, weight, gain, zs, ys):
    wide = master.shape[-1]
    width = -(-(wide // zs + LANES - TILE) // LANES) * LANES
    (first,) = pack_for(pack_first_kernel, 1, width, master, weight, gain, zs, ys)
    later = pack_for(pack_ringed_kernel, len(LATER), wide, master, weight, gain, zs, ys)
    near = dict(zip(LATER, later))
    near[RING[0]] = first
    return [near[dz] for dz in range(zs)]


def router_tiles_kernel(*refs):
    zs = len(refs) - 1
    z = lax.axis_index("z")
    for j in range(zs):
        refs[zs][lax.rem(z + zs - j, zs)] = refs[j][-TILE:, :]


def router_tiles(near):
    return pl.pallas_call(
        router_tiles_kernel,
        in_specs=[pl.BlockSpec((TILE, LANES), lambda e: (near[0].shape[0] // TILE - 1, 0))] * len(near),
        out_specs=VMEM,
        out_shape=packed((len(near), TILE, LANES)),
        grid=(1,),
        compiler_params=GRANT,
        name="router_tiles",
    )(*near)


def regroup_kernel(ys, *refs):
    count = len(refs) - ys
    y = lax.axis_index("y")
    rows = refs[count].shape[1]
    for k in range(ys):
        start = pl.multiple_of(lax.rem(y + k, ys) * rows, TILE)
        for n in range(count):
            refs[count + k][n] = refs[n][pl.ds(start, rows), :]


def regroup(near, ys):
    rows, lanes = near[0].shape
    shape = packed((len(near), (rows - TILE) // ys, lanes))
    return pl.pallas_call(
        functools.partial(regroup_kernel, ys),
        in_specs=[VMEM] * len(near),
        out_specs=[VMEM] * ys,
        out_shape=[shape] * ys,
        compiler_params=GRANT,
    )(*near)


def router_rows_kernel(*refs):
    out_ref = refs[-1]
    ys = len(refs) - 1
    y = lax.axis_index("y")

    def write(me):
        for even in range(0, ys, 2):
            a, b = (me - even) % ys, (me - even - 1) % ys
            for z in range(refs[0].shape[0]):
                first, second = refs[a][z], refs[b][z]
                column = (z * ys + even) * (LANES // 2)
                out_ref[:TILE, column : column + LANES] = jnp.concatenate(
                    [first[:, : LANES // 2], second[:, : LANES // 2]], axis=1
                )
                out_ref[TILE:, column : column + LANES] = jnp.concatenate(
                    [first[:, LANES // 2 :], second[:, LANES // 2 :]], axis=1
                )

    for me in range(ys):
        pl.when(y == me)(functools.partial(write, me))


def router_rows(tiles):
    zs, ys = tiles[0].shape[0], len(tiles)
    return pl.pallas_call(
        router_rows_kernel,
        in_specs=[VMEM] * ys,
        out_specs=VMEM,
        out_shape=packed((2 * TILE, zs * ys * LANES // 2)),
        compiler_params=GRANT,
        name="router_rows",
    )(*tiles)


def sent(out_ref, units_ref, sems, write):
    count, _, rows, _ = units_ref.shape
    copies = []
    for n in range(count):
        part = slice(n * rows, (n + 1) * rows)
        write(units_ref.at[n], part)
        copies.append(pltpu.make_async_copy(units_ref.at[n], out_ref.at[:, part], sems.at[n]))
        copies[-1].start()
    for copy in copies:
        copy.wait()


def unpack(kernel, operands, scratch, rows, depth):
    return pl.pallas_call(
        kernel,
        in_specs=[VMEM] * len(operands),
        out_specs=HBM,
        out_shape=pltpu.HBM((2, rows, depth), jnp.bfloat16),
        scratch_shapes=[
            *scratch,
            pltpu.VMEM((rows // CHUNK, 2, CHUNK, depth), jnp.bfloat16),
            pltpu.SemaphoreType.DMA((rows // CHUNK,)),
        ],
        compiler_params=GRANT,
        cost_estimate=cost(8 * rows * depth),
    )(*operands)


def unpack_ringed_kernel(*refs):
    groups, (out_ref, ordered_ref, units_ref, sems) = refs[:-4], refs[-4:]
    ys, zs = ordered_ref.shape[:2]
    z, y = lax.axis_index("z"), lax.axis_index("y")
    for n, group in enumerate(groups):
        for place, dz in enumerate(BATCHES[n // ys]):
            ordered_ref[lax.rem(y + ys - n % ys, ys), lax.rem(z + zs - dz, zs)] = group[place]

    def write(unit_ref, part):
        for z in range(zs):
            for even in range(0, ys, 2):
                column = (z * ys + even) * (LANES // 2)
                here, there = merged_pairs(ordered_ref[even, z, part, :], ordered_ref[even + 1, z, part, :])
                unit_ref[0, :, column : column + LANES] = here
                unit_ref[1, :, column : column + LANES] = there

    sent(out_ref, units_ref, sems, write)


def unpack_rest_kernel(in_ref, out_ref, units_ref, sems):
    def write(unit_ref, part):
        for k in range(in_ref.shape[0] // 2):
            here, there = merged_pairs(in_ref[2 * k, part, :], in_ref[2 * k + 1, part, :])
            unit_ref[0, :, k * LANES : (k + 1) * LANES] = here
            unit_ref[1, :, k * LANES : (k + 1) * LANES] = there

    sent(out_ref, units_ref, sems, write)


def pack_rest_kernel(shards, own, up_ref, out_ref, units_ref, rows_ref, sems, out_sems):
    copies = []
    half = up_ref.shape[1]
    for n, moved in fetched([up_ref.at[:, e] for e in range(half)], units_ref, sems):
        rows = slice(n * own, (n + 1) * own)
        rows_ref[:, rows, :] = moved.reshape(shards, own, LANES)
        copies.append(pltpu.make_async_copy(rows_ref.at[:, rows], out_ref.at[:, rows], out_sems.at[n]))
        copies[-1].start()
    for copy in copies:
        copy.wait()


def pack_rest(up, shards):
    _, half, depth, wide = up.shape
    own = wide // shards
    shape = (shards, half * own, LANES)
    return pl.pallas_call(
        functools.partial(pack_rest_kernel, shards, own),
        in_specs=[HBM],
        out_specs=HBM,
        out_shape=pltpu.HBM(shape, jnp.bfloat16),
        scratch_shapes=[
            pltpu.VMEM((half, 2, depth, wide), jnp.float32),
            pltpu.VMEM(shape, jnp.bfloat16),
            pltpu.SemaphoreType.DMA((half,)),
            pltpu.SemaphoreType.DMA((half,)),
        ],
        compiler_params=GRANT,
        cost_estimate=cost(6 * up.size),
        name="pack_rest",
    )(up)


def router_column_kernel(*refs):
    xs = len(refs) - 1
    x = lax.axis_index("x")
    for k in range(xs):
        refs[xs][lax.rem(x + xs - k, xs)] = refs[k][...]


def router_column(groups):
    return pl.pallas_call(
        router_column_kernel,
        in_specs=[VMEM] * len(groups),
        out_specs=VMEM,
        out_shape=packed((len(groups), *groups[0].shape)),
        compiler_params=GRANT,
        name="router_column",
    )(*groups)


def whole_router_kernel(mine_ref, other_ref, out_ref, rows_ref):
    xs, high, _ = mine_ref.shape
    core = lax.axis_index("core")
    for x in range(xs):
        for other, ref in enumerate((mine_ref, other_ref)):
            group = 2 * x + lax.rem(core + other, 2)
            rows_ref[pl.ds(pl.multiple_of(group * high, TILE), high), :] = ref[x]
    out_ref[...] = rows_ref[...].T


def whole_router(mine, other):
    xs, high, depth = mine.shape
    return pl.pallas_call(
        whole_router_kernel,
        in_specs=[VMEM] * 2,
        out_specs=VMEM,
        out_shape=packed((depth, 2 * xs * high)),
        scratch_shapes=[pltpu.VMEM((2 * xs * high, depth), jnp.bfloat16)],
        compiler_params=GRANT,
        name="whole_router",
    )(mine, other)


def in_hbm(array):
    return pltpu.with_memory_space_constraint(array, pltpu.HBM)


def shifted(block, axis, by):
    size = lax.axis_size(axis)
    return lax.ppermute(block, axis, [(k, (k + by) % size) for k in range(size)])


def per_device(master_gate, master_up, router_weight, router_gain):
    zs, ys = lax.axis_size("z"), lax.axis_size("y")
    experts, depth, wide = master_gate.shape
    half, own = experts // 2, wide // (zs * ys)
    gate, up = (m.reshape(2, half, depth, wide) for m in (master_gate, master_up))
    gate, up = in_hbm(gate), in_hbm(up)
    weight, gain = in_hbm(router_weight.T), in_hbm(router_gain[None])
    near = pack_ring(gate, weight, gain, zs, ys)
    for dz in RING:
        near[dz] = shifted(near[dz], "z", dz)
    rest = pack_rest(up, zs * ys)
    got_rest = lax.all_to_all(rest, SHARD, 0, 0, tiled=True)
    tiles = [router_tiles(near)] * ys
    for dy in SIDES:
        tiles[dy] = shifted(tiles[dy], "y", dy)
    groups = []
    for batch in BATCHES:
        group = list(regroup([near[dz] for dz in batch], ys))
        for dy in SIDES:
            group[dy] = shifted(group[dy], "y", dy)
        groups += group
    rows = router_rows(tiles)
    columns = [rows] * lax.axis_size("x")
    for dx in SIDES:
        columns[dx] = shifted(rows, "x", dx)
    column = router_column(columns)
    other = shifted(column, "core", 1)
    serve_router = whole_router(column, other)
    rows, width = half * own, zs * ys * depth
    ordered = [pltpu.VMEM((ys, zs, rows, LANES), jnp.bfloat16)]
    final_gate = unpack(unpack_ringed_kernel, groups, ordered, rows, width)
    final_up = unpack(unpack_rest_kernel, [got_rest], [], rows, width)
    whole = (experts, own, zs * ys * depth)
    return final_gate.reshape(whole), final_up.reshape(whole), serve_router


def solution(mesh):
    torus = Mesh(mesh.devices.reshape(4, 2, 8, 4), ("x", "core", "z", "y"))
    return jax.shard_map(
        per_device,
        mesh=torus,
        in_specs=(P(EXPERT, SHARD, None), P(EXPERT, SHARD, None), P(SHARD, EXPERT), P(SHARD)),
        out_specs=(P(EXPERT, SHARD, None), P(EXPERT, SHARD, None), P()),
        check_vma=False,
    )
```
